32 devices in a mesh: rep: 4 (over x, y), dp: 8 (over z, core).
Axes of the slice: x: 2, y: 2, z: 4, core: 2. Of those that a mesh axis runs over, the one named last changes fastest.
Arguments:
- g_w_gate: bfloat16 [32, 2, 1280, 5120], P(('rep', 'dp')), parts along dimension 0
- g_w_up: bfloat16 [32, 2, 1280, 5120], P(('rep', 'dp')), parts along dimension 0
- g_w_down: bfloat16 [32, 2, 5120, 1280], P(('rep', 'dp')), parts along dimension 0
- w_gate: bfloat16 [2, 1280, 5120], replicated
- w_up: bfloat16 [2, 1280, 5120], replicated
- w_down: bfloat16 [2, 5120, 1280], replicated
- m_w_gate: float32 [2, 1280, 5120], P(None, 'dp')
- m_w_up: float32 [2, 1280, 5120], P(None, 'dp')
- m_w_down: float32 [2, 5120, 1280], P(None, 'dp')
- v_w_gate: float32 [2, 1280, 5120], P(None, 'dp')
- v_w_up: float32 [2, 1280, 5120], P(None, 'dp')
- v_w_down: float32 [2, 5120, 1280], P(None, 'dp')
Outputs:
- output 1: bfloat16 [8, 1280, 5120], P('rep'), parts along dimension 0
- output 2: bfloat16 [8, 1280, 5120], P('rep'), parts along dimension 0
- output 3: bfloat16 [8, 5120, 1280], P('rep'), parts along dimension 0
- output 4: float32 [8, 1280, 5120], P('rep', 'dp'), parts along dimension 0
- output 5: float32 [8, 1280, 5120], P('rep', 'dp'), parts along dimension 0
- output 6: float32 [8, 5120, 1280], P('rep', 'dp'), parts along dimension 0
- output 7: float32 [8, 1280, 5120], P('rep', 'dp'), parts along dimension 0
- output 8: float32 [8, 1280, 5120], P('rep', 'dp'), parts along dimension 0
- output 9: float32 [8, 5120, 1280], P('rep', 'dp'), parts along dimension 0
There are 4 independent parts. The reference program is written for one: setup_inputs(seed, part) draws one part's arguments, and reference() takes and returns one part's arrays. A program takes and returns all parts, laid end to end along the dimension named above; an argument that names none is the same for every part.
All inputs are finite; a program needn't handle non-finite values.
Results may differ from the reference program's by a relative error of at most 0.022.
Values are sent between devices in bfloat16 or wider.
A program may use at most 2 GiB of HBM per device.

```python
import jax
import jax.numpy as jnp
from jax import lax

DEVICES = 8
D = 1280
FF = 5120
LAYERS = 2
NAMES = ("w_gate", "w_up", "w_down")
SHAPES = {"w_gate": (LAYERS, D, FF), "w_up": (LAYERS, D, FF), "w_down": (LAYERS, FF, D)}


def setup_inputs(seed: int = 0, part: int = 0) -> dict:
    kz, *keys = jax.random.split(jax.random.key(seed), 1 + 5 * len(NAMES))
    loud = 2.0 ** jax.random.uniform(kz, (), jnp.float32, -1.0, 1.0)
    drawn = {}
    for name, key, both in zip(NAMES, keys[:3], keys[3:6], strict=True):
        own = jax.random.normal(jax.random.fold_in(key, part), (DEVICES, *SHAPES[name]), jnp.float32)
        shared = jax.random.normal(jax.random.fold_in(both, part), SHAPES[name], jnp.float32)
        drawn["g_" + name] = (loud * (0.7 * shared / DEVICES + 0.7 * own * DEVICES**-0.5)).astype(jnp.bfloat16)
    for name, key in zip(NAMES, keys[6:9], strict=True):
        drawn[name] = (jax.random.normal(key, SHAPES[name], jnp.float32) * SHAPES[name][1] ** -0.5).astype(jnp.bfloat16)
    for name, key in zip(NAMES, keys[9:12], strict=True):
        drawn["m_" + name] = loud * 0.5 * jax.random.normal(key, SHAPES[name], jnp.float32)
    for name, key in zip(NAMES, keys[12:15], strict=True):
        drawn["v_" + name] = loud * loud * jax.random.uniform(key, SHAPES[name], jnp.float32, 0.5, 1.5)
    return drawn


def adamw(w, m, v, g):
    m = 0.9 * m + 0.1 * g
    v = 0.95 * v + 0.05 * g * g
    step = m * lax.rsqrt(v + 1e-8) + 0.1 * w
    return (w - 0.02 * step).astype(jnp.bfloat16), m, v


def clipped(gradients, sum_of_squares, count):
    factor = jnp.minimum(1.0, 0.5 * lax.rsqrt(sum_of_squares / count + 1e-30))
    return [g * factor for g in gradients]


def reference(g_w_gate, g_w_up, g_w_down, w_gate, w_up, w_down, m_w_gate, m_w_up, m_w_down, v_w_gate, v_w_up, v_w_down):
    def total(terms):
        return lax.scan(lambda so_far, term: (so_far + term.astype(jnp.float32), None), jnp.zeros(terms.shape[1:], jnp.float32), terms)[0]

    gradients = [total(terms).astype(jnp.bfloat16).astype(jnp.float32) for terms in (g_w_gate, g_w_up, g_w_down)]
    gradients = clipped(gradients, sum(jnp.sum(g * g) for g in gradients), sum(g.size for g in gradients))
    new = [
        adamw(w.astype(jnp.float32), m, v, g)
        for w, m, v, g in zip((w_gate, w_up, w_down), (m_w_gate, m_w_up, m_w_down), (v_w_gate, v_w_up, v_w_down), gradients, strict=True)
    ]
    return tuple(one[which] for which in range(3) for one in new)
```

```python
import functools

import jax
import jax.numpy as jnp
from jax import lax
from jax.experimental import pallas as pl
from jax.experimental.pallas import tpu as pltpu
from jax.sharding import PartitionSpec as P

MESH = pl.DeviceIdType.MESH
F32, BF16 = jnp.float32, jnp.bfloat16


def rows_of(x):
    *lead, r, c = x.shape
    n = len(lead)
    x = x.reshape(*lead, r // 8, 8, c // 128, 128).transpose(*range(n), n, n + 2, n + 1, n + 3)
    return x.reshape(*lead, r * c // 128, 128)


def from_rows(x, r, c):
    *lead, _, _ = x.shape
    n = len(lead)
    x = x.reshape(*lead, r // 8, c // 128, 8, 128).transpose(*range(n), n, n + 2, n + 1, n + 3)
    return x.reshape(*lead, r, c)


class Cfg:
    def __init__(self, rows, ch, skew, ch2, lag):
        self.R, self.CH, self.D, self.CH2, self.L = rows, ch, skew, ch2, lag
        self.SUB = rows // ch
        self.N = 12 * self.SUB
        self.SL = 4
        self.SP = 6
        self.SR = skew + 3
        self.SO = 3
        self.K2 = rows // ch2
        self.M = 6 * self.K2


def add_rows(refs, out, n, step, squares=None):
    def body(i, _):
        at = pl.ds(pl.multiple_of(i * step, step), step)
        total = refs[0][at].astype(F32)
        for r in refs[1:]:
            total = total + r[at].astype(F32)
        total = total.astype(BF16)
        out[at] = total
        if squares is not None:
            g = total.astype(F32)
            squares[...] += jnp.sum((g * g).reshape(step // 8, 8, 128), axis=0)
        return 0

    lax.fori_loop(0, n // step, body, 0)


def kernel(cfg, g0, g1, g2, w0, w1, w2, m0, m1, m2, v0, v1, v2, wt, g_own, g_fwd, factor, own, par, rin, out, sq, sq_in,
           gbuf, wbuf, mbuf, vbuf, nbuf, own_sem, ps, pr, rs, rr, par_credit, rin_credit, sqs, sqr,
           e_sem, c_sem, loc_sem, pown_sem, pfc, pfe, pr2, g1r, re, rc, ld_sem, gl_sem):
    R, CH, D, SUB, N = cfg.R, cfg.CH, cfg.D, cfg.SUB, cfg.N
    SL, SP, SR, SO, CH2, K2, M, L = cfg.SL, cfg.SP, cfg.SR, cfg.SO, cfg.CH2, cfg.K2, cfg.M, cfg.L
    g_in, w_in, m_in, v_in = (g0, g1, g2), (w0, w1, w2), (m0, m1, m2), (v0, v1, v2)
    me = lax.axis_index("dp")
    chip, k = me // 2, lax.rem(me, 2)
    half = chip // 2
    end = (chip == 0) | (chip == 3)
    mid = jnp.logical_not(end)
    my_end, my_mid = 3 * half, 1 + half
    far_mid, far_end = 2 - half, 3 - 3 * half
    partner = {"dp": me + 1 - 2 * k}
    to_c = {"dp": 2 * jnp.where(end, my_mid, far_mid) + k}
    to_e = {"dp": 2 * my_end + k}

    def remote(src, dst, send, recv, device):
        return pltpu.make_async_remote_copy(src_ref=src, dst_ref=dst, send_sem=send, recv_sem=recv, device_id=device, device_id_type=MESH)

    barrier = pltpu.get_barrier_semaphore()
    for i in range(1, 8):
        pl.semaphore_signal(barrier, inc=1, device_id={"dp": lax.rem(me + i, 8)}, device_id_type=MESH)
    pl.semaphore_wait(barrier, 7)

    sq[...] = jnp.zeros_like(sq)

    def block_of(s, b, lane):
        if s == 0:
            return 2 * jnp.where(b == 0, far_mid, far_end) + lane
        return 2 * jnp.where(b == 0, my_mid, my_end) + lane

    def split(i):
        p = i // SUB
        return p // 4, lax.rem(p // 2, 2), lax.rem(p, 2), lax.rem(i, SUB) * CH

    def of_weight(w, refs, do):
        for j in range(3):
            @pl.when(w == j)
            def _():
                do(refs[j])

    def term(ref, s, i, lane):
        w, l, b, off = split(i)
        return ref.at[l, pl.ds(pl.multiple_of(block_of(s, b, lane) * R + off, CH), CH)]

    def load_own(s, i):
        w = i // (4 * SUB)
        of_weight(w, g_in, lambda ref: pltpu.make_async_copy(term(ref, s, i, k), own.at[s, lax.rem(i, SL)], own_sem.at[s, lax.rem(i, SL)]).start())

    def wait_own(s, i):
        pltpu.make_async_copy(g_in[0].at[0, pl.ds(0, CH)], own.at[s, lax.rem(i, SL)], own_sem.at[s, lax.rem(i, SL)]).wait()

    def give(ref, s, i):
        j = lax.rem(i, SP)
        return remote(term(ref, s, i, 1 - k), par.at[s, j], ps.at[s, j], pr.at[s, j], partner)

    def send_given(s, i):
        of_weight(i // (4 * SUB), g_in, lambda ref: give(ref, s, i).start())

    def wait_given(s, i):
        give(g_in[0], s, lax.rem(i, SP)).wait_send()

    def wait_par(s, i):
        give(g_in[0], s, lax.rem(i, SP)).wait_recv()

    def forward(s, i, to_stream, device):
        j, o = lax.rem(i, SR), lax.rem(i, SO)
        return remote(out.at[s, o], rin.at[to_stream, j], rs.at[s, o], rr.at[to_stream, j], device)

    def keep(ref, i):
        w, l, b, off = split(i)
        o = lax.rem(i, SO)
        return pltpu.make_async_copy(out.at[1, o], ref.at[w, l, pl.ds(pl.multiple_of(off, CH), CH)], rs.at[1, o])

    for s in (0, 1):
        for i in range(SL):
            load_own(s, jnp.int32(i))
        for i in range(SP - 2):
            send_given(s, jnp.int32(i))

    def stream(s, i, arrives, leaves):
        wait_own(s, i)
        wait_par(s, i)
        refs = [own.at[s, lax.rem(i, SL)], par.at[s, lax.rem(i, SP)]]
        if arrives is not None:
            remote(out.at[s, 0], rin.at[s, lax.rem(i, SR)], rs.at[s, 0], rr.at[s, lax.rem(i, SR)], partner).wait_recv()
            refs.append(rin.at[s, lax.rem(i, SR)])

        @pl.when(i >= SO)
        def _():
            if leaves is None:
                keep(g_own, i - SO).wait()
            else:
                forward(s, i - SO, leaves[0], leaves[1]).wait_send()

        add_rows(refs, out.at[s, lax.rem(i, SO)], CH, cfg.step, sq if leaves is None else None)

        @pl.when(i + SP < N)
        def _():
            pl.semaphore_signal(par_credit.at[s], inc=1, device_id=partner, device_id_type=MESH)

        if arrives is not None:
            @pl.when(i + SR < N)
            def _():
                pl.semaphore_signal(rin_credit.at[arrives[0]], inc=1, device_id=arrives[1], device_id_type=MESH)

        if leaves is None:
            b = lax.rem(i // SUB, 2)

            @pl.when(b == 0)
            def _():
                keep(g_fwd, i).start()

            @pl.when(b == 1)
            def _():
                keep(g_own, i).start()
        else:
            @pl.when(i >= SR)
            def _():
                pl.semaphore_wait(rin_credit.at[s], 1)

            forward(s, i, leaves[0], leaves[1]).start()

        @pl.when(i + SL < N)
        def _():
            load_own(s, i + SL)

        j = i + SP - 2

        @pl.when(j < N)
        def _():
            @pl.when(j >= SP)
            def _():
                wait_given(s, j - SP)
                pl.semaphore_wait(par_credit.at[s], 1)

            send_given(s, j)

    def hand(t):
        p, off = t // K2, pl.multiple_of(lax.rem(t, K2) * CH2, CH2)
        at = (p // 2, lax.rem(p, 2), pl.ds(off, CH2))
        return remote(g_fwd.at[at], g_own.at[at], e_sem.at[lax.rem(t, 2)], g1r.at[t], to_c)

    def first(t, _):
        i0, i1 = t - jnp.where(end, 0, D), t - jnp.where(end, 3 * D, 2 * D)
        in0, in1 = (i0 >= 0) & (i0 < N), (i1 >= 0) & (i1 < N)

        @pl.when(end & in0)
        def _():
            stream(0, i0, None, (0, to_c))

        @pl.when(mid & in0)
        def _():
            stream(0, i0, (0, to_e), (1, to_c))

        @pl.when(mid & in1)
        def _():
            stream(1, i1, (0, to_c), (1, to_e))

        @pl.when(end & in1)
        def _():
            stream(1, i1, (1, to_c), None)

        @pl.when(end & (t == N + 1))
        def _():
            hand(jnp.int32(0)).start()

        return 0

    lax.fori_loop(0, N + 3 * D, first, 0)

    for i in range(N - SO, N):
        @pl.when(end)
        def _():
            forward(0, jnp.int32(i), 0, to_c).wait_send()
            keep(g_own, jnp.int32(i)).wait()

        @pl.when(mid)
        def _():
            forward(0, jnp.int32(i), 1, to_c).wait_send()
            forward(1, jnp.int32(i), 1, to_e).wait_send()

    part = 2 * half + k

    def tell(i):
        return remote(sq, sq_in.at[part], sqs.at[i], sqr.at[part], {"dp": lax.rem(me + i, 8)})

    @pl.when(end)
    def _():
        for i in (2, 6, 1, 3, 4, 5, 7):
            tell(i).start()

    def loads(t, slot):
        p, off = t // K2, pl.multiple_of(lax.rem(t, K2) * CH2, CH2)
        l = lax.rem(p, 2)

        def start(w):
            pltpu.make_async_copy(w_in[w].at[l, pl.ds(pl.multiple_of(me * R + off, CH2), CH2)], wbuf.at[slot], ld_sem.at[0, slot]).start()
            pltpu.make_async_copy(m_in[w].at[l, pl.ds(off, CH2)], mbuf.at[slot], ld_sem.at[1, slot]).start()
            pltpu.make_async_copy(v_in[w].at[l, pl.ds(off, CH2)], vbuf.at[slot], ld_sem.at[2, slot]).start()

        for w in range(3):
            @pl.when(p // 2 == w)
            def _():
                start(w)

    def wait_loads(slot):
        pltpu.make_async_copy(w_in[0].at[0, pl.ds(0, CH2)], wbuf.at[slot], ld_sem.at[0, slot]).wait()
        pltpu.make_async_copy(m_in[0].at[0, pl.ds(0, CH2)], mbuf.at[slot], ld_sem.at[1, slot]).wait()
        pltpu.make_async_copy(v_in[0].at[0, pl.ds(0, CH2)], vbuf.at[slot], ld_sem.at[2, slot]).wait()

    def load_g(t, slot):
        p, off = t // K2, pl.multiple_of(lax.rem(t, K2) * CH2, CH2)
        return pltpu.make_async_copy(g_own.at[p // 2, lax.rem(p, 2), pl.ds(off, CH2)], gbuf.at[slot], gl_sem.at[slot])

    loads(jnp.int32(0), jnp.int32(0))

    @pl.when(end)
    def _():
        load_g(jnp.int32(0), jnp.int32(0)).start()

    for j in range(4):
        @pl.when(end & (part == j))
        def _():
            sq_in[j] = sq[...]

        @pl.when(jnp.logical_not(end & (part == j)))
        def _():
            remote(sq, sq_in.at[j], sqs.at[0], sqr.at[j], partner).wait_recv()

    total = jnp.sum((sq_in[0] + sq_in[1]) + (sq_in[2] + sq_in[3]))
    factor[...] = jnp.minimum(1.0, 0.5 * lax.rsqrt(jnp.full((8, 128), total, F32) * (1.0 / (48.0 * R * 128)) + 1e-30))

    def at(t, dev):
        p = t // K2
        return wt.at[p // 2, lax.rem(p, 2), pl.ds(pl.multiple_of(dev * R + lax.rem(t, K2) * CH2, CH2), CH2)]

    def step_of(slot):
        n = cfg.step

        def body(i, _):
            r = pl.ds(pl.multiple_of(i * n, n), n)
            g = gbuf[slot, r].astype(F32).reshape(n // 8, 8, 128) * factor[...][None]
            w = wbuf[slot, r].astype(F32).reshape(n // 8, 8, 128)
            m = 0.9 * mbuf[slot, r].reshape(n // 8, 8, 128) + 0.1 * g
            v = 0.95 * vbuf[slot, r].reshape(n // 8, 8, 128) + 0.05 * g * g
            new = w - 0.02 * (m * lax.rsqrt(v + 1e-8) + 0.1 * w)
            nbuf[slot, r] = new.reshape(n, 128).astype(BF16)
            return 0

        lax.fori_loop(0, CH2 // n, body, 0)

    def to_partner(t, dev, sem):
        return remote(at(t, dev), at(t, dev), sem, pr2.at[t // (2 * K2)], partner)

    def own_to_partner(t):
        slot = lax.rem(t, 2)
        return remote(nbuf.at[slot], at(t, me), pown_sem.at[slot], pr2.at[t // (2 * K2)], partner)

    def own_to_wt(t):
        slot = lax.rem(t, 2)
        return pltpu.make_async_copy(nbuf.at[slot], at(t, me), loc_sem.at[slot])

    def end_send(u):
        return remote(at(u - M, me), at(u - M, me), e_sem.at[lax.rem(u, 2)], re.at[u - M], to_c)

    def end_phase(t, _):
        @pl.when(t < M)
        def _():
            slot = lax.rem(t, 2)

            @pl.when(t >= 2)
            def _():
                hand(t - 2).wait_send()

            @pl.when(t >= 1)
            def _():
                hand(t).start()

            @pl.when(t + 1 < M)
            def _():
                loads(t + 1, 1 - slot)
                load_g(t + 1, 1 - slot).start()

            wait_loads(slot)
            load_g(t, slot).wait()

            @pl.when(t >= 2)
            def _():
                own_to_wt(t - 2).wait()
                own_to_partner(t - 2).wait_send()

            step_of(slot)
            own_to_wt(t).start()
            own_to_partner(t).start()

            @pl.when(t == M - 1)
            def _():
                for j in (M - 2, M - 1):
                    own_to_wt(jnp.int32(j)).wait()
                    own_to_partner(jnp.int32(j)).wait_send()

        @pl.when((t >= M) & (t < 2 * M))
        def _():
            @pl.when(t < M + 2)
            def _():
                hand(t - 2).wait_send()

            @pl.when(t >= M + 2)
            def _():
                end_send(t - 2).wait_send()

            end_send(t).start()

        @pl.when((t >= 2 * M) & (t < 2 * M + 2))
        def _():
            end_send(t - 2).wait_send()

        q = t - L

        @pl.when(q >= 0)
        def _():
            c, j = q // M, lax.rem(q, M)
            dev = 2 * jnp.where(c == 0, my_mid, jnp.where(c == 1, far_mid, far_end)) + k
            remote(at(j, dev), at(j, dev), pfc.at[0], rc.at[q], partner).wait_recv()

            @pl.when(q >= 2)
            def _():
                to_partner(j, dev, pfc.at[lax.rem(q, 2)]).wait_send()

            to_partner(j, dev, pfc.at[lax.rem(q, 2)]).start()

        return 0

    def mid_own(t, there):
        slot = lax.rem(t, 2)
        if there == "e":
            return remote(nbuf.at[slot], at(t, me), e_sem.at[slot], rc.at[t], to_e)
        return remote(nbuf.at[slot], at(t, me), c_sem.at[slot], rc.at[t], to_c)

    def mid_to_end(u):
        j = lax.rem(u, M)
        dev = 2 * jnp.where(u < 2 * M, far_mid, far_end) + k
        return remote(at(j, dev), at(j, dev), e_sem.at[lax.rem(u, 2)], rc.at[u], to_e)

    def mid_across(q):
        dev = 2 * my_end + k
        return remote(at(q, dev), at(q, dev), c_sem.at[lax.rem(q, 2)], rc.at[M + q], to_c)

    def mid_phase(t, _):
        @pl.when(t < M)
        def _():
            slot = lax.rem(t, 2)

            @pl.when(t + 1 < M)
            def _():
                loads(t + 1, 1 - slot)

            hand(t).wait_recv()
            load_g(t, slot).start()
            wait_loads(slot)
            load_g(t, slot).wait()

            @pl.when(t >= 2)
            def _():
                own_to_wt(t - 2).wait()
                own_to_partner(t - 2).wait_send()
                mid_own(t - 2, "e").wait_send()
                mid_own(t - 2, "c").wait_send()

            step_of(slot)
            mid_own(t, "e").start()
            mid_own(t, "c").start()
            own_to_partner(t).start()
            own_to_wt(t).start()

        @pl.when((t >= M) & (t < M + 2))
        def _():
            own_to_wt(t - 2).wait()
            own_to_partner(t - 2).wait_send()
            mid_own(t - 2, "e").wait_send()
            mid_own(t - 2, "c").wait_send()

        @pl.when((t >= M) & (t < 3 * M))
        def _():
            @pl.when(t >= M + 2)
            def _():
                mid_to_end(t - 2).wait_send()

            mid_to_end(t).start()

        @pl.when(t >= 3 * M)
        def _():
            @pl.when(t < 3 * M + 2)
            def _():
                mid_to_end(t - 2).wait_send()

        e = t - M - L

        @pl.when((e >= 0) & (e < M))
        def _():
            dev = 2 * my_end + k
            remote(at(e, dev), at(e, dev), pfe.at[0], re.at[e], partner).wait_recv()

            @pl.when(e >= 2)
            def _():
                to_partner(e, dev, pfe.at[lax.rem(e, 2)]).wait_send()
                mid_across(e - 2).wait_send()

            mid_across(e).start()
            to_partner(e, dev, pfe.at[lax.rem(e, 2)]).start()

        @pl.when((e >= M) & (e < M + 2))
        def _():
            to_partner(e - 2, 2 * my_end + k, pfe.at[lax.rem(e, 2)]).wait_send()
            mid_across(e - 2).wait_send()

        q = t - 2 * L

        @pl.when((q >= 0) & (q < 2 * M))
        def _():
            j = lax.rem(q, M)
            dev = 2 * jnp.where(q < M, far_mid, far_end) + k
            remote(at(j, dev), at(j, dev), pfc.at[0], rc.at[q], partner).wait_recv()

            @pl.when(q >= 2)
            def _():
                to_partner(j, dev, pfc.at[lax.rem(q, 2)]).wait_send()

            to_partner(j, dev, pfc.at[lax.rem(q, 2)]).start()

        return 0

    @pl.when(end)
    def _():
        lax.fori_loop(0, 3 * M + L, end_phase, 0)

    @pl.when(mid)
    def _():
        lax.fori_loop(0, 3 * M + 2, mid_phase, 0)

    for j in range(2):
        to_partner(jnp.int32(0), me, pfc.at[j]).wait_send()
    for s in (0, 1):
        for i in range(N - SP, N):
            wait_given(s, jnp.int32(i))

    @pl.when(end)
    def _():
        for i in range(1, 8):
            tell(i).wait_send()

    for w in range(3):
        half_of = wt.at[w, :, pl.ds(0, 4 * R)]
        pltpu.make_async_copy(half_of, half_of, pr2.at[w]).wait()


def sum_step_gather(cfg, terms, weights, m, v):
    R, DMA, REG = cfg.R, pltpu.SemaphoreType.DMA, pltpu.SemaphoreType.REGULAR
    CH, CH2, SL, SP, SR, SO, M = cfg.CH, cfg.CH2, cfg.SL, cfg.SP, cfg.SR, cfg.SO, cfg.M
    anywhere = pl.BlockSpec(memory_space=pl.ANY)
    return pl.pallas_call(
        functools.partial(kernel, cfg),
        name="sum_step_gather",
        out_shape=(
            jax.ShapeDtypeStruct((3, 2, 8 * R, 128), BF16),
            jax.ShapeDtypeStruct((3, 2, R, 128), BF16),
            jax.ShapeDtypeStruct((3, 2, R, 128), BF16),
            jax.ShapeDtypeStruct((8, 128), F32),
        ),
        in_specs=[anywhere] * 12,
        out_specs=(anywhere, anywhere, anywhere, pl.BlockSpec(memory_space=pltpu.VMEM)),
        scratch_shapes=[
            pltpu.VMEM((2, SL, CH, 128), BF16),
            pltpu.VMEM((2, SP, CH, 128), BF16),
            pltpu.VMEM((2, SR, CH, 128), BF16),
            pltpu.VMEM((2, SO, CH, 128), BF16),
            pltpu.VMEM((8, 128), F32),
            pltpu.VMEM((4, 8, 128), F32),
            pltpu.VMEM((2, CH2, 128), BF16),
            pltpu.VMEM((2, CH2, 128), BF16),
            pltpu.VMEM((2, CH2, 128), F32),
            pltpu.VMEM((2, CH2, 128), F32),
            pltpu.VMEM((2, CH2, 128), BF16),
            DMA((2, SL)),
            DMA((2, SP)),
            DMA((2, SP)),
            DMA((2, SO)),
            DMA((2, SR)),
            REG((2,)),
            REG((2,)),
            DMA((8,)),
            DMA((4,)),
            DMA((2,)),
            DMA((2,)),
            DMA((2,)),
            DMA((2,)),
            DMA((2,)),
            DMA((2,)),
            DMA((3,)),
            DMA((M,)),
            DMA((M,)),
            DMA((3 * M,)),
            DMA((3, 2)),
            DMA((2,)),
        ],
        compiler_params=pltpu.CompilerParams(collective_id=0, has_side_effects=True, vmem_limit_bytes=60 * 2**20),
    )(*terms, *weights, *m, *v)


def solution(mesh):
    def step(*arrays):
        terms, weights, m, v = (arrays[i : i + 3] for i in (0, 3, 6, 9))
        rows = m[0].shape[1] * m[0].shape[2] // 128
        cfg = Cfg(rows, ch=rows // 16, skew=3, ch2=rows // 4, lag=4)
        cfg.step = min(cfg.CH, 80)
        wt, g_own, _, factor = sum_step_gather(
            cfg,
            [rows_of(t[0]) for t in terms],
            [rows_of(w) for w in weights],
            [rows_of(x) for x in m],
            [rows_of(x) for x in v],
        )
        whole = [from_rows(wt[j], *w.shape[1:]) for j, w in enumerate(weights)]
        new_m, new_v = [], []
        for j in range(3):
            g = from_rows(g_own[j], *m[j].shape[1:]).astype(F32) * factor[0, 0]
            new_m.append(0.9 * m[j] + 0.1 * g)
            new_v.append(0.95 * v[j] + 0.05 * g * g)
        return (*whole, *new_m, *new_v)

    all_of, cut = P(None, None, None), P(None, "dp", None)
    return jax.shard_map(
        step,
        mesh=mesh,
        in_specs=(P(("rep", "dp"), None, None, None),) * 3 + (all_of,) * 3 + (cut,) * 6,
        out_specs=(P("rep", None, None),) * 3 + (P("rep", "dp", None),) * 6,
        check_vma=False,
    )
```

```python
import functools

import jax
import jax.numpy as jnp
from jax import lax
from jax.experimental import pallas as pl
from jax.experimental.pallas import tpu as pltpu
from jax.sharding import PartitionSpec as P

MESH = pl.DeviceIdType.MESH
F32, BF16 = jnp.float32, jnp.bfloat16


def rows_of(x):
    *lead, r, c = x.shape
    n = len(lead)
    x = x.reshape(*lead, r // 8, 8, c // 128, 128).transpose(*range(n), n, n + 2, n + 1, n + 3)
    return x.reshape(*lead, r * c // 128, 128)


def from_rows(x, r, c):
    *lead, _, _ = x.shape
    n = len(lead)
    x = x.reshape(*lead, r // 8, c // 128, 8, 128).transpose(*range(n), n, n + 2, n + 1, n + 3)
    return x.reshape(*lead, r, c)


class Cfg:
    def __init__(self, rows, ch, skew, ch2, lag):
        self.R, self.CH, self.D, self.CH2, self.L = rows, ch, skew, ch2, lag
        self.SUB = rows // ch
        self.N = 12 * self.SUB
        self.SL = 4
        self.SP = 6
        self.SR = skew + 3
        self.SO = 3
        self.K2 = rows // ch2
        self.M = 6 * self.K2


def add_rows(refs, out, n, step, squares=None):
    def body(i, _):
        at = pl.ds(pl.multiple_of(i * step, step), step)
        total = refs[0][at].astype(F32)
        for r in refs[1:]:
            total = total + r[at].astype(F32)
        total = total.astype(BF16)
        out[at] = total
        if squares is not None:
            g = total.astype(F32)
            squares[...] += jnp.sum((g * g).reshape(step // 8, 8, 128), axis=0)
        return 0

    lax.fori_loop(0, n // step, body, 0)


def kernel(cfg, g0, g1, g2, w0, w1, w2, m0, m1, m2, v0, v1, v2, wt, g_own, g_fwd, factor, late0, late1, plate0, plate1, own, par, rin, out, sq, sq_in,
           gbuf, wbuf, mbuf, vbuf, nbuf, own_sem, ps, pr, rs, rr, par_credit, rin_credit, sqs, sqr,
           e_sem, c_sem, loc_sem, pown_sem, pfc, pfe, pr2, plr, g1r, re, rc, ld_sem, gl_sem):
    R, CH, D, SUB, N = cfg.R, cfg.CH, cfg.D, cfg.SUB, cfg.N
    SL, SP, SR, SO, CH2, K2, M, L = cfg.SL, cfg.SP, cfg.SR, cfg.SO, cfg.CH2, cfg.K2, cfg.M, cfg.L
    late, plate = (late0, late1), (plate0, plate1)
    T = 2 * K2
    first_late = M - T
    g_in, w_in, m_in, v_in = (g0, g1, g2), (w0, w1, w2), (m0, m1, m2), (v0, v1, v2)
    me = lax.axis_index("dp")
    chip, k = me // 2, lax.rem(me, 2)
    half = chip // 2
    end = (chip == 0) | (chip == 3)
    mid = jnp.logical_not(end)
    my_end, my_mid = 3 * half, 1 + half
    far_mid, far_end = 2 - half, 3 - 3 * half
    partner = {"dp": me + 1 - 2 * k}
    to_c = {"dp": 2 * jnp.where(end, my_mid, far_mid) + k}
    to_e = {"dp": 2 * my_end + k}

    def remote(src, dst, send, recv, device):
        return pltpu.make_async_remote_copy(src_ref=src, dst_ref=dst, send_sem=send, recv_sem=recv, device_id=device, device_id_type=MESH)

    barrier = pltpu.get_barrier_semaphore()
    for i in range(1, 8):
        pl.semaphore_signal(barrier, inc=1, device_id={"dp": lax.rem(me + i, 8)}, device_id_type=MESH)
    pl.semaphore_wait(barrier, 7)

    sq[...] = jnp.zeros_like(sq)

    def block_of(s, b, lane):
        if s == 0:
            return 2 * jnp.where(b == 0, far_mid, far_end) + lane
        return 2 * jnp.where(b == 0, my_mid, my_end) + lane

    def split(i):
        p = i // SUB
        return p // 4, lax.rem(p // 2, 2), lax.rem(p, 2), lax.rem(i, SUB) * CH

    def of_weight(w, refs, do):
        for j in range(3):
            @pl.when(w == j)
            def _():
                do(refs[j])

    def term(ref, s, i, lane):
        w, l, b, off = split(i)
        return ref.at[l, pl.ds(pl.multiple_of(block_of(s, b, lane) * R + off, CH), CH)]

    def load_own(s, i):
        w = i // (4 * SUB)
        of_weight(w, g_in, lambda ref: pltpu.make_async_copy(term(ref, s, i, k), own.at[s, lax.rem(i, SL)], own_sem.at[s, lax.rem(i, SL)]).start())

    def wait_own(s, i):
        pltpu.make_async_copy(g_in[0].at[0, pl.ds(0, CH)], own.at[s, lax.rem(i, SL)], own_sem.at[s, lax.rem(i, SL)]).wait()

    def give(ref, s, i):
        j = lax.rem(i, SP)
        return remote(term(ref, s, i, 1 - k), par.at[s, j], ps.at[s, j], pr.at[s, j], partner)

    def send_given(s, i):
        of_weight(i // (4 * SUB), g_in, lambda ref: give(ref, s, i).start())

    def wait_given(s, i):
        give(g_in[0], s, lax.rem(i, SP)).wait_send()

    def wait_par(s, i):
        give(g_in[0], s, lax.rem(i, SP)).wait_recv()

    def forward(s, i, to_stream, device):
        j, o = lax.rem(i, SR), lax.rem(i, SO)
        return remote(out.at[s, o], rin.at[to_stream, j], rs.at[s, o], rr.at[to_stream, j], device)

    def keep(ref, i):
        w, l, b, off = split(i)
        o = lax.rem(i, SO)
        return pltpu.make_async_copy(out.at[1, o], ref.at[w, l, pl.ds(pl.multiple_of(off, CH), CH)], rs.at[1, o])

    for s in (0, 1):
        for i in range(SL):
            load_own(s, jnp.int32(i))
        for i in range(SP - 2):
            send_given(s, jnp.int32(i))

    def stream(s, i, arrives, leaves):
        wait_own(s, i)
        wait_par(s, i)
        refs = [own.at[s, lax.rem(i, SL)], par.at[s, lax.rem(i, SP)]]
        if arrives is not None:
            remote(out.at[s, 0], rin.at[s, lax.rem(i, SR)], rs.at[s, 0], rr.at[s, lax.rem(i, SR)], partner).wait_recv()
            refs.append(rin.at[s, lax.rem(i, SR)])

        @pl.when(i >= SO)
        def _():
            if leaves is None:
                keep(g_own, i - SO).wait()
            else:
                forward(s, i - SO, leaves[0], leaves[1]).wait_send()

        add_rows(refs, out.at[s, lax.rem(i, SO)], CH, cfg.step, sq if leaves is None else None)

        @pl.when(i + SP < N)
        def _():
            pl.semaphore_signal(par_credit.at[s], inc=1, device_id=partner, device_id_type=MESH)

        if arrives is not None:
            @pl.when(i + SR < N)
            def _():
                pl.semaphore_signal(rin_credit.at[arrives[0]], inc=1, device_id=arrives[1], device_id_type=MESH)

        if leaves is None:
            b = lax.rem(i // SUB, 2)

            @pl.when(b == 0)
            def _():
                keep(g_fwd, i).start()

            @pl.when(b == 1)
            def _():
                keep(g_own, i).start()
        else:
            @pl.when(i >= SR)
            def _():
                pl.semaphore_wait(rin_credit.at[s], 1)

            forward(s, i, leaves[0], leaves[1]).start()

        @pl.when(i + SL < N)
        def _():
            load_own(s, i + SL)

        j = i + SP - 2

        @pl.when(j < N)
        def _():
            @pl.when(j >= SP)
            def _():
                wait_given(s, j - SP)
                pl.semaphore_wait(par_credit.at[s], 1)

            send_given(s, j)

    def hand(t):
        p, off = t // K2, pl.multiple_of(lax.rem(t, K2) * CH2, CH2)
        at = (p // 2, lax.rem(p, 2), pl.ds(off, CH2))
        return remote(g_fwd.at[at], g_own.at[at], e_sem.at[lax.rem(t, 2)], g1r.at[t], to_c)

    def first(t, _):
        i0, i1 = t - jnp.where(end, 0, D), t - jnp.where(end, 3 * D, 2 * D)
        in0, in1 = (i0 >= 0) & (i0 < N), (i1 >= 0) & (i1 < N)

        @pl.when(end & in0)
        def _():
            stream(0, i0, None, (0, to_c))

        @pl.when(mid & in0)
        def _():
            stream(0, i0, (0, to_e), (1, to_c))

        @pl.when(mid & in1)
        def _():
            stream(1, i1, (0, to_c), (1, to_e))

        @pl.when(end & in1)
        def _():
            stream(1, i1, (1, to_c), None)

        @pl.when(end & (t == N + 1))
        def _():
            hand(jnp.int32(0)).start()

        return 0

    lax.fori_loop(0, N + 3 * D, first, 0)

    for i in range(N - SO, N):
        @pl.when(end)
        def _():
            forward(0, jnp.int32(i), 0, to_c).wait_send()
            keep(g_own, jnp.int32(i)).wait()

        @pl.when(mid)
        def _():
            forward(0, jnp.int32(i), 1, to_c).wait_send()
            forward(1, jnp.int32(i), 1, to_e).wait_send()

    part = 2 * half + k

    def tell(i):
        return remote(sq, sq_in.at[part], sqs.at[i], sqr.at[part], {"dp": lax.rem(me + i, 8)})

    @pl.when(end)
    def _():
        for i in (2, 6, 1, 3, 4, 5, 7):
            tell(i).start()

    def loads(t, slot):
        p, off = t // K2, pl.multiple_of(lax.rem(t, K2) * CH2, CH2)
        l = lax.rem(p, 2)

        def start(w):
            pltpu.make_async_copy(w_in[w].at[l, pl.ds(pl.multiple_of(me * R + off, CH2), CH2)], wbuf.at[slot], ld_sem.at[0, slot]).start()
            pltpu.make_async_copy(m_in[w].at[l, pl.ds(off, CH2)], mbuf.at[slot], ld_sem.at[1, slot]).start()
            pltpu.make_async_copy(v_in[w].at[l, pl.ds(off, CH2)], vbuf.at[slot], ld_sem.at[2, slot]).start()

        for w in range(3):
            @pl.when(p // 2 == w)
            def _():
                start(w)

    def wait_loads(slot):
        pltpu.make_async_copy(w_in[0].at[0, pl.ds(0, CH2)], wbuf.at[slot], ld_sem.at[0, slot]).wait()
        pltpu.make_async_copy(m_in[0].at[0, pl.ds(0, CH2)], mbuf.at[slot], ld_sem.at[1, slot]).wait()
        pltpu.make_async_copy(v_in[0].at[0, pl.ds(0, CH2)], vbuf.at[slot], ld_sem.at[2, slot]).wait()

    def load_g(t, slot):
        p, off = t // K2, pl.multiple_of(lax.rem(t, K2) * CH2, CH2)
        return pltpu.make_async_copy(g_own.at[p // 2, lax.rem(p, 2), pl.ds(off, CH2)], gbuf.at[slot], gl_sem.at[slot])

    loads(jnp.int32(0), jnp.int32(0))

    @pl.when(end)
    def _():
        load_g(jnp.int32(0), jnp.int32(0)).start()

    for j in range(4):
        @pl.when(end & (part == j))
        def _():
            sq_in[j] = sq[...]

        @pl.when(jnp.logical_not(end & (part == j)))
        def _():
            remote(sq, sq_in.at[j], sqs.at[0], sqr.at[j], partner).wait_recv()

    total = jnp.sum((sq_in[0] + sq_in[1]) + (sq_in[2] + sq_in[3]))
    factor[...] = jnp.minimum(1.0, 0.5 * lax.rsqrt(jnp.full((8, 128), total, F32) * (1.0 / (48.0 * R * 128)) + 1e-30))

    def at(t, dev):
        p = t // K2
        return wt.at[p // 2, lax.rem(p, 2), pl.ds(pl.multiple_of(dev * R + lax.rem(t, K2) * CH2, CH2), CH2)]

    def step_of(slot):
        n = cfg.step

        def body(i, _):
            r = pl.ds(pl.multiple_of(i * n, n), n)
            g = gbuf[slot, r].astype(F32).reshape(n // 8, 8, 128) * factor[...][None]
            w = wbuf[slot, r].astype(F32).reshape(n // 8, 8, 128)
            m = 0.9 * mbuf[slot, r].reshape(n // 8, 8, 128) + 0.1 * g
            v = 0.95 * vbuf[slot, r].reshape(n // 8, 8, 128) + 0.05 * g * g
            new = w - 0.02 * (m * lax.rsqrt(v + 1e-8) + 0.1 * w)
            nbuf[slot, r] = new.reshape(n, 128).astype(BF16)
            return 0

        lax.fori_loop(0, CH2 // n, body, 0)

    def to_partner(t, dev, sem):
        return remote(at(t, dev), at(t, dev), sem, pr2.at[t // (2 * K2)], partner)

    def late_at(refs, j, do):
        off = pl.multiple_of(lax.rem(j, K2) * CH2, CH2)
        for l in range(2):
            @pl.when((j - first_late) // K2 == l)
            def _():
                do([r[l].at[pl.ds(off, CH2)] for r in refs])

    def own_to_partner(t):
        slot = lax.rem(t, 2)
        return remote(nbuf.at[slot], at(t, me), pown_sem.at[slot], pr2.at[t // (2 * K2)], partner)

    def own_to_wt(t):
        slot = lax.rem(t, 2)
        return pltpu.make_async_copy(nbuf.at[slot], at(t, me), loc_sem.at[slot])

    def end_send(u):
        return remote(at(u - M, me), at(u - M, me), e_sem.at[lax.rem(u, 2)], re.at[u - M], to_c)

    def end_phase(t, _):
        @pl.when(t < M)
        def _():
            slot = lax.rem(t, 2)

            @pl.when(t >= 2)
            def _():
                hand(t - 2).wait_send()

            @pl.when(t >= 1)
            def _():
                hand(t).start()

            @pl.when(t + 1 < M)
            def _():
                loads(t + 1, 1 - slot)
                load_g(t + 1, 1 - slot).start()

            wait_loads(slot)
            load_g(t, slot).wait()

            @pl.when(t >= 2)
            def _():
                own_to_wt(t - 2).wait()
                own_to_partner(t - 2).wait_send()

            step_of(slot)
            own_to_wt(t).start()
            own_to_partner(t).start()

            @pl.when(t == M - 1)
            def _():
                for j in (M - 2, M - 1):
                    own_to_wt(jnp.int32(j)).wait()
                    own_to_partner(jnp.int32(j)).wait_send()

        @pl.when((t >= M) & (t < 2 * M))
        def _():
            @pl.when(t < M + 2)
            def _():
                hand(t - 2).wait_send()

            @pl.when(t >= M + 2)
            def _():
                end_send(t - 2).wait_send()

            end_send(t).start()

        @pl.when((t >= 2 * M) & (t < 2 * M + 2))
        def _():
            end_send(t - 2).wait_send()

        q = t - L

        @pl.when(q >= 0)
        def _():
            c, j = q // M, lax.rem(q, M)
            dev = 2 * jnp.where(c == 0, my_mid, jnp.where(c == 1, far_mid, far_end)) + k
            remote(at(j, dev), at(j, dev), pfc.at[0], rc.at[q], partner).wait_recv()

            @pl.when(q >= 2)
            def _():
                to_partner(j, dev, pfc.at[lax.rem(q, 2)]).wait_send()

            to_partner(j, dev, pfc.at[lax.rem(q, 2)]).start()

        return 0

    def mid_own(t, there):
        slot = lax.rem(t, 2)
        if there == "e":
            return remote(nbuf.at[slot], at(t, me), e_sem.at[slot], rc.at[t], to_e)
        return remote(nbuf.at[slot], at(t, me), c_sem.at[slot], rc.at[t], to_c)

    def mid_to_end(u):
        j = lax.rem(u, M)
        dev = 2 * jnp.where(u < 2 * M, far_mid, far_end) + k
        return remote(at(j, dev), at(j, dev), e_sem.at[lax.rem(u, 2)], rc.at[u], to_e)

    def mid_across(q, place=None):
        dev = 2 * my_end + k
        return remote(at(q, dev), at(q, dev) if place is None else place, c_sem.at[lax.rem(q, 2)], rc.at[M + q], to_c)

    def mid_phase(t, _):
        @pl.when(t < M)
        def _():
            slot = lax.rem(t, 2)

            @pl.when(t + 1 < M)
            def _():
                loads(t + 1, 1 - slot)

            hand(t).wait_recv()
            load_g(t, slot).start()
            wait_loads(slot)
            load_g(t, slot).wait()

            @pl.when(t >= 2)
            def _():
                own_to_wt(t - 2).wait()
                own_to_partner(t - 2).wait_send()
                mid_own(t - 2, "e").wait_send()
                mid_own(t - 2, "c").wait_send()

            step_of(slot)
            mid_own(t, "e").start()
            mid_own(t, "c").start()
            own_to_partner(t).start()
            own_to_wt(t).start()

        @pl.when((t >= M) & (t < M + 2))
        def _():
            own_to_wt(t - 2).wait()
            own_to_partner(t - 2).wait_send()
            mid_own(t - 2, "e").wait_send()
            mid_own(t - 2, "c").wait_send()

        @pl.when((t >= M) & (t < 3 * M - T))
        def _():
            @pl.when(t >= M + 2)
            def _():
                mid_to_end(t - 2).wait_send()

            mid_to_end(t).start()

        @pl.when((t >= 3 * M - T) & (t < 3 * M - T + 2))
        def _():
            mid_to_end(t - 2).wait_send()

        e = t - M - L

        @pl.when((e >= 0) & (e < M))
        def _():
            dev = 2 * my_end + k
            remote(at(e, dev), at(e, dev), pfe.at[0], re.at[e], partner).wait_recv()

            @pl.when(e >= 2)
            def _():
                to_partner(e, dev, pfe.at[lax.rem(e, 2)]).wait_send()
                mid_across(e - 2).wait_send()

            @pl.when(e < first_late)
            def _():
                mid_across(e).start()

            @pl.when(e >= first_late)
            def _():
                late_at([late], e, lambda p: mid_across(e, p[0]).start())

            to_partner(e, dev, pfe.at[lax.rem(e, 2)]).start()

        @pl.when((e >= M) & (e < M + 2))
        def _():
            to_partner(e - 2, 2 * my_end + k, pfe.at[lax.rem(e, 2)]).wait_send()
            mid_across(e - 2).wait_send()

        q = t - 2 * L

        @pl.when((q >= 0) & (q < 2 * M))
        def _():
            j = lax.rem(q, M)
            dev = 2 * jnp.where(q < M, far_mid, far_end) + k
            sem = pfc.at[lax.rem(q, 2)]
            remote(at(j, dev), at(j, dev), pfc.at[0], rc.at[q], partner).wait_recv()

            @pl.when(q >= 2)
            def _():
                to_partner(j, dev, sem).wait_send()

            @pl.when(q < 2 * M - T)
            def _():
                to_partner(j, dev, sem).start()

            @pl.when(q >= 2 * M - T)
            def _():
                late_at([late, plate], j, lambda p: remote(p[0], p[1], sem, plr.at[0], partner).start())

        return 0

    @pl.when(end)
    def _():
        lax.fori_loop(0, 3 * M - T + L, end_phase, 0)

    @pl.when(mid)
    def _():
        lax.fori_loop(0, max(3 * M - T + 2, 2 * M + 2 * L), mid_phase, 0)

    for j in range(2):
        to_partner(jnp.int32(0), me, pfc.at[j]).wait_send()
    for s in (0, 1):
        for i in range(N - SP, N):
            wait_given(s, jnp.int32(i))

    @pl.when(end)
    def _():
        for i in range(1, 8):
            tell(i).wait_send()

    for w in range(3):
        all_given = wt.at[w, :, pl.ds(0, (4 if w < 2 else 3) * R)]
        pltpu.make_async_copy(all_given, all_given, pr2.at[w]).wait()

    @pl.when(mid)
    def _():
        given = wt.at[0, :, pl.ds(0, R)]
        pltpu.make_async_copy(given, given, plr.at[0]).wait()


def outputs(rows, factor, wt, g, m, v, w_out, m_out, v_out):
    w_out[...] = wt[...]

    def body(i, _):
        r = pl.ds(pl.multiple_of(i * rows, rows), rows)
        grad = g[r].astype(F32).reshape(rows // 8, 8, 128) * factor[...][None]
        new_m = 0.9 * m[r].reshape(rows // 8, 8, 128) + 0.1 * grad
        new_v = 0.95 * v[r].reshape(rows // 8, 8, 128) + 0.05 * grad * grad
        m_out[r] = new_m.reshape(rows, 128)
        v_out[r] = new_v.reshape(rows, 128)
        return 0

    lax.fori_loop(0, g.shape[0] // rows, body, 0)


def write_outputs(cfg, j, factor, wt, g_own, m, v):
    R = cfg.R
    parts = 8

    def share(n, *lead):
        return pl.BlockSpec((*(None,) * (len(lead) + 1), n, 128), lambda l, i: (*lead, l, i, 0))

    big, small = R, R // parts
    moment = jax.ShapeDtypeStruct((2, R, 128), F32)
    return pl.pallas_call(
        functools.partial(outputs, cfg.step),
        name="write_outputs",
        grid=(2, parts),
        in_specs=[pl.BlockSpec((8, 128), lambda l, i: (0, 0)), share(big, j), share(small, j), share(small), share(small)],
        out_specs=(share(big), share(small), share(small)),
        out_shape=(jax.ShapeDtypeStruct((2, 8 * R, 128), BF16), moment, moment),
        cost_estimate=pl.CostEstimate(flops=2 * 10**10, bytes_accessed=(64 + 2 * 18) * R * 128, transcendentals=0),
    )(factor, wt, g_own, m, v)


def insert(layer, R, here, given, mine, yours, _, w_out, buf, ld, st):
    me = lax.axis_index("dp")
    chip, k = me // 2, lax.rem(me, 2)
    end = (chip == 0) | (chip == 3)
    far_end = 3 - 3 * (chip // 2)
    n, c = 4, R // 4
    steps = [(s, i) for i in range(n) for s in range(2)]

    def load(ref, s, i):
        return pltpu.make_async_copy(ref.at[pl.ds(i * c, c)], buf.at[s, pl.ds(i * c, c)], ld.at[s, i])

    def store(s, i):
        dev = 2 * far_end + (k if s == 0 else 1 - k)
        return pltpu.make_async_copy(buf.at[s, pl.ds(i * c, c)], w_out.at[layer, pl.ds(pl.multiple_of(dev * R + i * c, c), c)], st.at[s, i])

    @pl.when(end)
    def _():
        for s, i in steps:
            load((here, given)[s], s, i).start()

    @pl.when(jnp.logical_not(end))
    def _():
        for s, i in steps:
            load((mine, yours)[s], s, i).start()

    for s, i in steps:
        load(here, s, i).wait()
        store(s, i).start()
    for s, i in steps:
        store(s, i).wait()


def insert_late(cfg, layer, here, given, mine, yours, whole):
    R = cfg.R
    anywhere = pl.BlockSpec(memory_space=pl.ANY)
    return pl.pallas_call(
        functools.partial(insert, layer, R),
        name="insert_late",
        in_specs=[anywhere] * 5,
        out_specs=anywhere,
        out_shape=jax.ShapeDtypeStruct(whole.shape, whole.dtype),
        scratch_shapes=[pltpu.VMEM((2, R, 128), BF16), pltpu.SemaphoreType.DMA((2, 4)), pltpu.SemaphoreType.DMA((2, 4))],
        input_output_aliases={4: 0},
        cost_estimate=pl.CostEstimate(flops=10**9, bytes_accessed=8 * R * 128, transcendentals=0),
    )(here, given, mine, yours, whole)


def sum_step_gather(cfg, terms, weights, m, v):
    R, DMA, REG = cfg.R, pltpu.SemaphoreType.DMA, pltpu.SemaphoreType.REGULAR
    CH, CH2, SL, SP, SR, SO, M = cfg.CH, cfg.CH2, cfg.SL, cfg.SP, cfg.SR, cfg.SO, cfg.M
    anywhere = pl.BlockSpec(memory_space=pl.ANY)
    return pl.pallas_call(
        functools.partial(kernel, cfg),
        name="sum_step_gather",
        out_shape=(
            jax.ShapeDtypeStruct((3, 2, 8 * R, 128), BF16),
            jax.ShapeDtypeStruct((3, 2, R, 128), BF16),
            jax.ShapeDtypeStruct((3, 2, R, 128), BF16),
            jax.ShapeDtypeStruct((8, 128), F32),
            *[jax.ShapeDtypeStruct((R, 128), BF16)] * 4,
        ),
        in_specs=[anywhere] * 12,
        out_specs=(anywhere, anywhere, anywhere, pl.BlockSpec(memory_space=pltpu.VMEM), *[anywhere] * 4),
        scratch_shapes=[
            pltpu.VMEM((2, SL, CH, 128), BF16),
            pltpu.VMEM((2, SP, CH, 128), BF16),
            pltpu.VMEM((2, SR, CH, 128), BF16),
            pltpu.VMEM((2, SO, CH, 128), BF16),
            pltpu.VMEM((8, 128), F32),
            pltpu.VMEM((4, 8, 128), F32),
            pltpu.VMEM((2, CH2, 128), BF16),
            pltpu.VMEM((2, CH2, 128), BF16),
            pltpu.VMEM((2, CH2, 128), F32),
            pltpu.VMEM((2, CH2, 128), F32),
            pltpu.VMEM((2, CH2, 128), BF16),
            DMA((2, SL)),
            DMA((2, SP)),
            DMA((2, SP)),
            DMA((2, SO)),
            DMA((2, SR)),
            REG((2,)),
            REG((2,)),
            DMA((8,)),
            DMA((4,)),
            DMA((2,)),
            DMA((2,)),
            DMA((2,)),
            DMA((2,)),
            DMA((2,)),
            DMA((2,)),
            DMA((3,)),
            DMA((1,)),
            DMA((M,)),
            DMA((M,)),
            DMA((3 * M,)),
            DMA((3, 2)),
            DMA((2,)),
        ],
        compiler_params=pltpu.CompilerParams(collective_id=0, has_side_effects=True, vmem_limit_bytes=60 * 2**20),
    )(*terms, *weights, *m, *v)


def solution(mesh):
    def step(*arrays):
        terms, weights, m, v = (arrays[i : i + 3] for i in (0, 3, 6, 9))
        rows = m[0].shape[1] * m[0].shape[2] // 128
        cfg = Cfg(rows, ch=rows // 16, skew=3, ch2=rows // 4, lag=4)
        cfg.step = min(cfg.CH, 80)
        rm, rv = [rows_of(x) for x in m], [rows_of(x) for x in v]
        wt, g_own, _, factor, late0, late1, plate0, plate1 = sum_step_gather(
            cfg, [rows_of(t[0]) for t in terms], [rows_of(w) for w in weights], rm, rv
        )
        to_end, swap = [(2, 0), (3, 1), (4, 6), (5, 7)], [(0, 1), (1, 0), (6, 7), (7, 6)]
        here = [lax.ppermute(x, "dp", to_end) for x in (late0, late1)]
        new = [write_outputs(cfg, j, factor, wt, g_own, rm[j], rv[j]) for j in range(3)]
        given = [lax.ppermute(x, "dp", swap) for x in here]
        down = new[2][0]
        for l, (mine, yours) in enumerate(((late0, plate0), (late1, plate1))):
            down = insert_late(cfg, l, here[l], given[l], mine, yours, down)
        whole = [from_rows(x, *w.shape[1:]) for x, w in zip((new[0][0], new[1][0], down), weights, strict=True)]
        new_m = [from_rows(one[1], *x.shape[1:]) for one, x in zip(new, m, strict=True)]
        new_v = [from_rows(one[2], *x.shape[1:]) for one, x in zip(new, v, strict=True)]
        return (*whole, *new_m, *new_v)

    all_of, cut = P(None, None, None), P(None, "dp", None)
    return jax.shard_map(
        step,
        mesh=mesh,
        in_specs=(P(("rep", "dp"), None, None, None),) * 3 + (all_of,) * 3 + (cut,) * 6,
        out_specs=(P("rep", None, None),) * 3 + (P("rep", "dp", None),) * 6,
        check_vma=False,
    )
```
